32 devices in a mesh: grp: 2 (over y), ep: 8 (over z, x), tp: 2 (over core).
Axes of the slice: x: 2, y: 2, z: 4, core: 2. Of those that a mesh axis runs over, the one named last changes fastest.
Arguments:
- queries: bfloat16 [1024, 16, 576], P(('grp', 'ep'), 'tp'), parts along dimension 0, may hold values from -450 to 450
- latent_cache: bfloat16 [48, 512, 576], P(('grp', 'ep'), 'tp'), parts along dimension 0, may hold values from -6 to 6
- residual: bfloat16 [1024, 2048], P(('grp', 'ep')), parts along dimension 0, may hold values from -8 to 8
- token_request: int32 [1024], P(('grp', 'ep')), parts along dimension 0, may hold values from 0 to 2, as said below
- token_visible: int32 [1024], P(('grp', 'ep')), parts along dimension 0, may hold values from 1 to 512, as said below
- value_proj: bfloat16 [16, 512, 128], P('tp', 'ep'), may hold values from -0.25 to 0.25
- out_proj: bfloat16 [2048, 2048], P('tp', 'ep'), may hold values from -0.125 to 0.125
- norm_gain: float32 [2048], replicated, may hold values from 0.1 to 1.9
- router: bfloat16 [2048, 64], replicated, may hold values from -0.0390625 to 0.0390625
- expert_ids: int32 [1024, 6], P(('grp', 'ep')), parts along dimension 0, may hold values from 0 to 63, all different within a row; in each aligned block of 64 rows (0 to 63, 64 to 127, ...) at most 8 rows name the same one
- gate_weight: bfloat16 [128, 2048, 384], P('ep', None, 'tp'), may hold values from -0.125 to 0.125
- up_weight: bfloat16 [128, 2048, 384], P('ep', None, 'tp'), may hold values from -0.125 to 0.125
- down_weight: bfloat16 [128, 384, 2048], P('ep', 'tp'), may hold values from -0.21875 to 0.21875
Outputs:
- hidden: bfloat16 [1024, 2048], P(('grp', 'ep'), 'tp'), parts along dimension 0
- expert_out: bfloat16 [1024, 2048], P(('grp', 'ep'), 'tp'), parts along dimension 0
The draws below stay inside these ranges and needn't reach their ends.
There are 2 independent parts, one for each index of `grp`. The reference program is written for one: setup_inputs(seed, part) draws one part's arguments, and reference() takes and returns one part's arrays. A program takes and returns all parts, laid end to end along the dimension named above; an argument that names none is the same for every part. Nothing has to cross between parts.
Inputs may be any that keep to these rules, and one draw needn't show every extreme that they name: `token_request`: in each ep block, 62 tokens belong to request 0, a prefill span, and each other request has exactly one token; the tokens' order in the block is arbitrary. `token_visible`: the span's tokens read consecutive counts s + 1 to s + 62; 512 is reached in every draw. `expert_ids`: each row names 6 different experts; among the 64 tokens of one ep index no expert is named by more than 8 tokens, and this bound is reached.
All inputs are finite; a program needn't handle non-finite values.
Results may differ from the reference program's by a relative error of at most 0.018.
Values may be sent and summed in bfloat16 or wider, within the bound.
No kernel may reach another device: no remote copies, remote signals or barrier semaphores. Data moves between devices by JAX's collectives and lax.ppermute only.
A program may use at most 128 MiB of HBM per device.

```python
import math
import jax
import jax.numpy as jnp
import numpy as np
from jax import lax

D = 2048
HEADS = 16
LATENT = 512
ROPE = 64
VDIM = 128
EXPERTS = 64
TOPK = 6
EXP_HIDDEN = 768
GROUPS = 2
TOK_DEV = 64
REQ_DEV = 3
CACHE_LEN = 512
CAP = 8
PIECES = 128
TOKENS = 512
REQS = 24
N_EP = 8
N_TP = 2


def request_layout(key):
    blocks = TOKENS // TOK_DEV
    prefill = TOK_DEV - REQ_DEV + 1
    streams = jax.random.split(jax.random.fold_in(key, 101), blocks)

    def one_block(stream, block_index):
        first, second, third = jax.random.split(stream, 3)
        ordering = jax.random.permutation(first, TOK_DEV).astype(jnp.int32)
        span_start = jax.random.randint(second, (), 0, CACHE_LEN - prefill + 1)
        lengths = jax.random.randint(third, (REQ_DEV - 1,), 1, CACHE_LEN + 1)
        lengths = jnp.where((block_index == 0) & (jnp.arange(REQ_DEV - 1) == 0), CACHE_LEN, lengths)
        in_span = ordering < prefill
        request = jnp.where(in_span, 0, ordering - prefill + 1)
        decode_index = jnp.clip(ordering - prefill, 0, REQ_DEV - 2)
        visible = jnp.where(in_span, span_start + ordering + 1, lengths[decode_index])
        return (request.astype(jnp.int32), visible.astype(jnp.int32))
    request, visible = jax.vmap(one_block)(streams, jnp.arange(blocks))
    return (request.reshape(TOKENS), visible.reshape(TOKENS))


def draw_token_request(key, part):
    return request_layout(key)[0]


def draw_token_visible(key, part):
    return request_layout(key)[1]


def cache_rope(key):
    return jnp.clip(jax.random.normal(jax.random.fold_in(key, 202), (REQS, CACHE_LEN, ROPE)), -4.0, 4.0)


def draw_latent_cache(key, part):
    latent = jnp.clip(jax.random.normal(jax.random.fold_in(key, 201), (REQS, CACHE_LEN, LATENT)), -4.0, 4.0)
    return jnp.concatenate([latent, cache_rope(key)], axis=2).astype(jnp.bfloat16)


def draw_queries(key, part):
    shape = (TOKENS, HEADS, LATENT + ROPE)
    values = 0.6 * jnp.clip(jax.random.normal(jax.random.fold_in(key, 301), shape), -4.0, 4.0)
    return values.astype(jnp.bfloat16)


def draw_residual(key, part):
    scales = jnp.exp(jax.random.uniform(jax.random.fold_in(key, 401), (TOKENS, 1), minval=jnp.log(0.2), maxval=jnp.log(2.0)))
    noise = jnp.clip(jax.random.normal(jax.random.fold_in(key, 402), (TOKENS, D)), -4.0, 4.0)
    return (scales * noise).astype(jnp.bfloat16)


def steps_of(own_key, extent, pieces, least, top_value):
    def one(dim, shards_of):
        heights = jax.random.uniform(jax.random.fold_in(jax.random.fold_in(own_key, 6), dim), (shards_of,), jnp.float32, least / len(pieces), top_value / len(pieces))
        return jnp.repeat(jnp.exp(heights), extent[dim] // shards_of).reshape((-1,) + (1,) * (len(extent) - dim - 1))

    level = one(*pieces[0])
    for cut in pieces[1:]:
        level = level * one(*cut)
    return level


def deal_out(stream_key, own, number, rows, count, top, most, skew):
    order = jax.random.permutation(stream_key, count)
    heavy_load, usual = portions_of(count, rows * top, most, skew, True), portions_of(count, rows * top, most, skew, False)
    places = jnp.arange(count)

    def named(tallies, offset_by):
        used = int((tallies > 0).sum())
        fixed = max(1, used // 4)
        moved = fixed + (places - fixed + offset_by * (used - fixed)) % max(1, count - fixed)
        return jnp.zeros((count,), jnp.int32).at[order[jnp.where(places < fixed, places, moved)]].set(jnp.asarray(tallies, jnp.int32))

    tallies = jnp.where(number % 4 == 0, named(heavy_load, number // 4), named(usual, number - number // 4 - 1))
    mixed = jax.random.permutation(jax.random.fold_in(own, 3), count)
    source_of, taker = mixed[0:count // 2 * 2:2], mixed[1:count // 2 * 2:2]
    margin = jnp.minimum(tallies[source_of] - 1, most - tallies[taker]) // 2
    margin = jnp.where((source_of == order[0]) | (taker == order[0]) | (tallies[taker] == 0), 0, jnp.maximum(margin, 0))
    moved = jax.random.randint(jax.random.fold_in(own, 4), (count // 2,), 0, 1 << 20) % (margin + 1)
    tallies = tallies.at[source_of].add(-moved).at[taker].add(moved)
    items = jnp.searchsorted(jnp.cumsum(tallies), jnp.arange(rows * top), side="right").astype(jnp.int32)
    grid = items.reshape(top, rows).T
    grid = grid[jax.random.permutation(jax.random.fold_in(own, 1), rows)]
    offset_by = jax.random.randint(jax.random.fold_in(own, 2), (rows, 1), 0, top)
    return jnp.take_along_axis(grid, (jnp.arange(top)[None, :] + offset_by) % top, axis=1)


def portions_of(amount, total, reach, lean, full):
    loads = [(1 << 20) // math.isqrt(grade ** lean) + 1 for grade in range(1, amount + 1)]
    largest = reach if full else min(reach, max(-(-total // amount), total * loads[0] // sum(loads)))
    least = 1 if total - largest >= amount - 1 else 0
    given, surplus = [largest] + [least] * (amount - 1), total - largest - least * (amount - 1)
    while surplus > 0:
        movable = [i for i in range(1, amount) if given[i] < largest] or [i for i in range(1, amount) if given[i] < reach]
        mass, remaining = sum([loads[i] for i in movable]), surplus
        for i in movable:
            more = min(reach - given[i], max(1, remaining * loads[i] // mass), surplus)
            given[i] = given[i] + more
            surplus = surplus - more
    return np.array(given)


def bell_draw(stream_key, shape, width, most, cuts=(), held_as=jnp.bfloat16):
    gain = steps_of(stream_key, shape, cuts, -0.22, 0.18) if cuts else 1.0
    array = jax.random.normal(stream_key, shape, jnp.float32) * width * gain
    return jnp.minimum(jnp.maximum(array, -most), most).astype(held_as)


def setup_inputs(seed: int = 0, part: int = 0) -> dict:
    key_of = jax.random.split(jax.random.key(seed), 14)
    part_keys = jax.random.split(jax.random.fold_in(key_of[13], part), 14)
    queries = draw_queries(jax.random.fold_in(jax.random.fold_in(key_of[13], part), 71), part)
    latent_cache = draw_latent_cache(jax.random.fold_in(jax.random.fold_in(key_of[13], part), 71), part)
    residual = draw_residual(jax.random.fold_in(jax.random.fold_in(key_of[13], part), 71), part)
    token_request = draw_token_request(jax.random.fold_in(jax.random.fold_in(key_of[13], part), 71), part)
    token_visible = draw_token_visible(jax.random.fold_in(jax.random.fold_in(key_of[13], part), 71), part)
    value_proj = bell_draw(key_of[5], (HEADS, LATENT, VDIM), LATENT ** -0.5, 0.25, ((0, 2), (1, 8)))
    out_proj = bell_draw(key_of[6], (HEADS * VDIM, D), (HEADS * VDIM) ** -0.5, 0.125, ((0, 2), (1, 8)))
    norm_gain = jnp.clip(1.0 + 0.18 * jax.random.normal(key_of[7], (D,), jnp.float32), 0.1, 1.9)
    router = bell_draw(key_of[8], (D, EXPERTS), (12 * D) ** -0.5, 0.0390625)
    expert_ids_keys = jax.random.split(jax.random.fold_in(part_keys[9], 1), TOKENS // TOK_DEV)
    expert_ids_turns = jax.random.permutation(jax.random.fold_in(part_keys[9], 3), TOKENS // TOK_DEV)
    expert_ids = jax.vmap(lambda own, number: deal_out(jax.random.fold_in(part_keys[9], 2), own, number, TOK_DEV, EXPERTS, TOPK, CAP, 2))(expert_ids_keys, expert_ids_turns).reshape((TOKENS, TOPK))
    gate_weight = bell_draw(key_of[10], (PIECES, D, EXP_HIDDEN // GROUPS), D ** -0.5, 0.125, ((0, 8), (2, 2)))
    up_weight = bell_draw(key_of[11], (PIECES, D, EXP_HIDDEN // GROUPS), D ** -0.5, 0.125, ((0, 8), (2, 2)))
    down_weight = bell_draw(key_of[12], (PIECES, EXP_HIDDEN // GROUPS, D), EXP_HIDDEN ** -0.5, 0.21875, ((0, 8), (1, 2)))
    return {"queries": queries, "latent_cache": latent_cache, "residual": residual, "token_request": token_request, "token_visible": token_visible, "value_proj": value_proj, "out_proj": out_proj, "norm_gain": norm_gain, "router": router, "expert_ids": expert_ids, "gate_weight": gate_weight, "up_weight": up_weight, "down_weight": down_weight}


score_scale = 192.0 ** (-0.5)
epsilon = 1e-06

def attend_block(arrays):
    queries, block_rows, token_request, token_visible = arrays
    per_request = block_rows.shape[1]
    flat_rows = block_rows.reshape(-1, block_rows.shape[2]).astype(jnp.float32)
    scores = jnp.einsum('thc,kc->thk', queries.astype(jnp.float32), flat_rows) * score_scale
    column = jnp.arange(flat_rows.shape[0], dtype=jnp.int32)
    owner_id = column // per_request
    position = column % per_request
    allowed = (owner_id[None, :] == token_request[:, None]) & (position[None, :] < token_visible[:, None])
    scores = jnp.where(allowed[:, None, :], scores, -jnp.inf)
    row_peak = lax.optimization_barrier(jnp.max(scores, axis=2, keepdims=True))
    rounded = lax.optimization_barrier(jnp.exp(scores - row_peak).astype(jnp.bfloat16))
    weights = rounded.astype(jnp.float32)
    totals = lax.optimization_barrier(jnp.sum(weights, axis=2, keepdims=True))
    summed = jnp.einsum('thk,kc->thc', weights, flat_rows[:, :LATENT])
    return (summed / totals).astype(jnp.bfloat16)

def reference(queries, latent_cache, residual, token_request, token_visible, value_proj, out_proj, norm_gain, router, expert_ids, gate_weight, up_weight, down_weight):
    blocks = TOKENS // TOK_DEV
    context = lax.map(attend_block, (queries.reshape(blocks, TOK_DEV, HEADS, LATENT + ROPE), latent_cache.reshape(blocks, REQ_DEV, CACHE_LEN, LATENT + ROPE), token_request.reshape(blocks, TOK_DEV), token_visible.reshape(blocks, TOK_DEV)))
    context = context.reshape(TOKENS, HEADS, LATENT)
    heads_out = jnp.einsum('thl,hlv->thv', context.astype(jnp.float32), value_proj.astype(jnp.float32)).astype(jnp.bfloat16)
    heads_out = heads_out.reshape(TOKENS, HEADS * VDIM)
    attention = jnp.dot(heads_out, out_proj, preferred_element_type=jnp.float32)
    hidden = (residual.astype(jnp.float32) + attention).astype(jnp.bfloat16)
    hidden_wide = hidden.astype(jnp.float32)
    normed = (hidden_wide * lax.rsqrt(lax.optimization_barrier(jnp.mean(hidden_wide * hidden_wide, axis=1, keepdims=True)) + epsilon) * norm_gain).astype(jnp.bfloat16)
    logits = jnp.dot(normed, router, preferred_element_type=jnp.float32)
    gate_share = jax.nn.softmax(jnp.take_along_axis(logits, expert_ids, axis=1), axis=1).astype(jnp.bfloat16)
    flat_ids = expert_ids.reshape(-1)
    flat_share = gate_share.reshape(-1).astype(jnp.float32)
    bound = N_EP * CAP
    part_width = EXP_HIDDEN // (GROUPS * N_TP)

    def piece_step(running, piece_index):
        expert = piece_index // GROUPS
        hit_mask = flat_ids == expert
        hits = jnp.nonzero(hit_mask, size=bound, fill_value=0)[0].astype(jnp.int32)
        live = jnp.arange(bound, dtype=jnp.int32) < jnp.sum(hit_mask.astype(jnp.int32))
        token_rows = hits // TOPK
        picked = normed[token_rows]
        gate_vals = jnp.dot(picked, gate_weight[piece_index], preferred_element_type=jnp.float32)
        up_vals = jnp.dot(picked, up_weight[piece_index], preferred_element_type=jnp.float32)
        activated = (jax.nn.silu(gate_vals) * up_vals).astype(jnp.bfloat16)
        combined = jnp.zeros((bound, D), jnp.float32)
        for half_index in range(N_TP):
            lower = half_index * part_width
            piece_out = jnp.dot(activated[:, lower:lower + part_width], down_weight[piece_index, lower:lower + part_width], preferred_element_type=jnp.float32).astype(jnp.bfloat16)
            combined = combined + piece_out.astype(jnp.float32)
        scaled = combined * jnp.where(live, flat_share[hits], 0.0)[:, None]
        return (running.at[token_rows].add(scaled), None)
    routed, _ = lax.scan(piece_step, jnp.zeros((TOKENS, D), jnp.float32), jnp.arange(PIECES, dtype=jnp.int32))
    return (hidden, routed.astype(jnp.bfloat16))
```

```python
import jax
import jax.numpy as jnp
from jax import lax
from jax.sharding import PartitionSpec as P

LATENT = 512
VDIM = 128
EXPERTS = 64
TOPK = 6
GROUPS = 2
CAP = 8
PIECES = 128


score_scale = 192.0 ** (-0.5)
epsilon = 1e-06


def masked_scores(queries, block_rows, token_request, token_visible):
    per_request = block_rows.shape[1]
    flat_rows = block_rows.reshape(-1, block_rows.shape[2])
    scores = (
        jnp.einsum("thc,kc->thk", queries, flat_rows, preferred_element_type=jnp.float32)
        * score_scale
    )
    column = jnp.arange(flat_rows.shape[0], dtype=jnp.int32)
    owner_id = column // per_request
    position = column % per_request
    allowed = (owner_id[None, :] == token_request[:, None]) & (
        position[None, :] < token_visible[:, None]
    )
    return (jnp.where(allowed[:, None, :], scores, -jnp.inf), flat_rows)


def weighted_rows(scores, row_peak, flat_rows):
    weights = jnp.exp(scores - row_peak[:, :, None]).astype(jnp.bfloat16)
    totals = jnp.sum(weights.astype(jnp.float32), axis=2)
    summed = jnp.einsum(
        "thk,kc->thc", weights, flat_rows[:, :LATENT], preferred_element_type=jnp.float32
    )
    return (summed, totals)


def expert_block(arrived, gate_weight, up_weight, down_weight):
    gate_vals = jnp.einsum("prd,pdf->prf", arrived, gate_weight, preferred_element_type=jnp.float32)
    up_vals = jnp.einsum("prd,pdf->prf", arrived, up_weight, preferred_element_type=jnp.float32)
    activated = (jax.nn.silu(gate_vals) * up_vals).astype(jnp.bfloat16)
    return jnp.einsum(
        "prf,pfd->prd", activated, down_weight, preferred_element_type=jnp.float32
    ).astype(jnp.bfloat16)


def wide_body(
    queries,
    latent_cache,
    residual,
    token_request,
    token_visible,
    value_proj,
    out_proj,
    norm_gain,
    router,
    expert_ids,
    gate_weight,
    up_weight,
    down_weight,
):
    all_rows = lax.all_gather(latent_cache, "tp", axis=1, tiled=True)
    scores, flat_rows = masked_scores(queries, all_rows, token_request, token_visible)
    summed, totals = weighted_rows(scores, jnp.max(scores, axis=2), flat_rows)
    context = (summed / totals[:, :, None]).astype(jnp.bfloat16)
    tokens_here = context.shape[0]
    heads_here = context.shape[1]
    head_values = jnp.einsum(
        "thl,hlv->thv",
        context,
        lax.all_gather(value_proj, "ep", axis=1, tiled=True),
        preferred_element_type=jnp.float32,
    )
    heads_out = head_values.astype(jnp.bfloat16).reshape(tokens_here, heads_here * VDIM)
    column_block = jnp.dot(
        lax.all_gather(heads_out, "ep", axis=0, tiled=True),
        out_proj,
        preferred_element_type=jnp.float32,
    )
    attention_part = lax.all_to_all(column_block, "ep", split_axis=0, concat_axis=1, tiled=True)
    attention = lax.psum(attention_part, "tp")
    hidden = (residual.astype(jnp.float32) + attention).astype(jnp.bfloat16)
    hidden_wide = hidden.astype(jnp.float32)
    normed = (
        hidden_wide
        * lax.rsqrt(jnp.mean(hidden_wide * hidden_wide, axis=1, keepdims=True) + epsilon)
        * norm_gain
    ).astype(jnp.bfloat16)
    logits = jnp.dot(normed, router, preferred_element_type=jnp.float32)
    gate_share = jax.nn.softmax(jnp.take_along_axis(logits, expert_ids, axis=1), axis=1).astype(
        jnp.bfloat16
    )
    flat_ids = expert_ids.reshape(-1)
    position_id = jnp.arange(flat_ids.shape[0], dtype=jnp.int32)
    earlier = (flat_ids[:, None] == flat_ids[None, :]) & (
        position_id[None, :] < position_id[:, None]
    )
    slot_ids = (flat_ids * CAP + jnp.sum(earlier.astype(jnp.int32), axis=1)).reshape(
        tokens_here, TOPK
    )
    targets = jnp.arange(EXPERTS * CAP, dtype=jnp.int32)
    matches = slot_ids[:, :, None] == targets[None, None, :]
    picker = jnp.any(matches, axis=1).T.astype(jnp.bfloat16)
    model_width = normed.shape[1]
    mixing = jnp.sum(
        jnp.where(matches, gate_share[:, :, None], jnp.zeros((), jnp.bfloat16)), axis=1
    )
    mixing = jnp.broadcast_to(
        mixing.reshape(tokens_here, EXPERTS, 1, CAP), (tokens_here, EXPERTS, GROUPS, CAP)
    ).reshape(tokens_here, PIECES * CAP)
    core_count = lax.axis_size("tp")
    half_width = model_width // core_count
    core_start = lax.axis_index("tp") * half_width
    outgoing = jnp.dot(picker, normed, preferred_element_type=jnp.float32).astype(jnp.bfloat16)
    outgoing = jnp.broadcast_to(
        outgoing.reshape(EXPERTS, 1, CAP, model_width), (EXPERTS, GROUPS, CAP, model_width)
    ).reshape(PIECES, CAP, model_width)
    arrived = lax.all_to_all(outgoing, "ep", split_axis=0, concat_axis=1, tiled=True)
    partial_out = expert_block(arrived, gate_weight, up_weight, down_weight)
    returned = lax.all_to_all(partial_out, "ep", split_axis=1, concat_axis=0, tiled=True)
    routed = jnp.dot(
        mixing, returned.reshape(PIECES * CAP, model_width), preferred_element_type=jnp.float32
    )
    expert_out = lax.psum_scatter(
        routed.astype(jnp.bfloat16), "tp", scatter_dimension=1, tiled=True
    )
    hidden_part = lax.dynamic_slice_in_dim(hidden, core_start, half_width, 1)
    return (hidden_part, expert_out)


def relative_blocks(block, width):
    pairs = lambda k: [(i, i ^ k) for i in range(width)]
    blocks = [None] * width
    blocks[0] = block
    order = sorted(range(2, width, 2), key=lambda k: -k.bit_length())
    for k in order:
        blocks[k] = lax.ppermute(block, "ep", pairs(k))
    for k in [0] + order:
        blocks[k + 1] = lax.ppermute(blocks[k], "ep", pairs(1))
    return blocks


def pick_block(stacked, index):
    return lax.dynamic_index_in_dim(stacked, index, 0, keepdims=False)


def gather_blocks(block, axis, width, place):
    stacked = jnp.stack(relative_blocks(block, width))
    return jnp.concatenate([pick_block(stacked, place ^ j) for j in range(width)], axis=axis)


def swap_cores(value):
    return lax.ppermute(value, "tp", [(0, 1), (1, 0)])


def experts_mixed(arrived, gate_weight, up_weight, down_weight, mixing):
    gate_vals = jnp.einsum(
        "xrd,xgdf->xgrf", arrived, gate_weight, preferred_element_type=jnp.float32
    )
    up_vals = jnp.einsum("xrd,xgdf->xgrf", arrived, up_weight, preferred_element_type=jnp.float32)
    activated = (jax.nn.silu(gate_vals) * up_vals).astype(jnp.bfloat16)
    slots_out = jnp.einsum(
        "xgrf,xgfd->xrd", activated, down_weight, preferred_element_type=jnp.float32
    ).astype(jnp.bfloat16)
    return jnp.dot(
        mixing, slots_out.reshape(-1, slots_out.shape[2]), preferred_element_type=jnp.float32
    )


def body(
    queries,
    latent_cache,
    residual,
    token_request,
    token_visible,
    value_proj,
    out_proj,
    norm_gain,
    router,
    expert_ids,
    gate_weight,
    up_weight,
    down_weight,
):
    width = lax.axis_size("ep")
    place = lax.axis_index("ep")
    core = lax.axis_index("tp")
    tokens_here, model_width = residual.shape
    all_tokens = tokens_here * width
    columns = out_proj.shape[1]
    half_columns = columns // 2
    half_width = model_width // 2

    other_rows = swap_cores(latent_cache)
    requests, positions, latent_width = latent_cache.shape
    value_full = gather_blocks(value_proj, 1, width, place)

    residual_blocks = residual.reshape(tokens_here, width, 2, half_columns)
    ids_wide = expert_ids.astype(jnp.bfloat16)
    sent = [
        lax.dynamic_slice(
            residual_blocks, (0, place ^ k, core, 0), (tokens_here, 1, 1, half_columns)
        ).reshape(tokens_here, half_columns)
        for k in range(width)
    ]
    early = [sent[0]] + [
        lax.ppermute(sent[k], "ep", [(i, i ^ k) for i in range(width)]) for k in range(1, width)
    ]
    early = jnp.stack(early)
    residual_columns = jnp.concatenate(
        [pick_block(early, place ^ j) for j in range(width)], axis=0
    )
    ids_all = gather_blocks(ids_wide, 0, width, place).astype(jnp.int32)

    flat_rows = jnp.concatenate([latent_cache, other_rows], axis=0).reshape(-1, latent_width)
    scores = (
        jnp.einsum("thc,kc->thk", queries, flat_rows, preferred_element_type=jnp.float32)
        * score_scale
    )
    column = jnp.arange(flat_rows.shape[0], dtype=jnp.int32)
    source_core = (column // (requests * positions)) ^ core
    owner_id = (column // positions) % requests
    position = column % positions + source_core * positions
    allowed = (owner_id[None, :] == token_request[:, None]) & (
        position[None, :] < token_visible[:, None]
    )
    scores = jnp.where(allowed[:, None, :], scores, -jnp.inf)
    summed, totals = weighted_rows(scores, jnp.max(scores, axis=2), flat_rows)
    context = (summed / totals[:, :, None]).astype(jnp.bfloat16)
    heads_here = context.shape[1]
    head_values = jnp.einsum(
        "thl,hlv->thv", context, value_full, preferred_element_type=jnp.float32
    )
    heads_out = head_values.astype(jnp.bfloat16).reshape(tokens_here, heads_here * VDIM)
    heads_all = gather_blocks(heads_out, 0, width, place)

    column_block = jnp.dot(heads_all, out_proj, preferred_element_type=jnp.float32)
    kept = lax.dynamic_slice_in_dim(column_block, core * half_columns, half_columns, 1)
    given = lax.dynamic_slice_in_dim(column_block, (1 - core) * half_columns, half_columns, 1)
    hidden_columns = (
        residual_columns.astype(jnp.float32) + (kept + swap_cores(given))
    ).astype(jnp.bfloat16)

    own_half = relative_blocks(hidden_columns, width)
    other_half = [swap_cores(block) for block in own_half]
    halves = jnp.stack(own_half + other_half)
    hidden = jnp.concatenate(
        [
            pick_block(halves, (place ^ j) + width * (core ^ side))
            for j in range(width)
            for side in range(2)
        ],
        axis=1,
    )
    hidden_part = lax.dynamic_slice(
        hidden, (place * tokens_here, core * half_width), (tokens_here, half_width)
    )
    hidden_wide = hidden.astype(jnp.float32)
    normed = (
        hidden_wide
        * lax.rsqrt(jnp.mean(hidden_wide * hidden_wide, axis=1, keepdims=True) + epsilon)
        * norm_gain
    ).astype(jnp.bfloat16)

    experts_here = gate_weight.shape[0] // GROUPS
    slots = CAP * width
    logits = jnp.dot(normed, router, preferred_element_type=jnp.float32)
    experts = jnp.arange(EXPERTS, dtype=jnp.int32)
    named = jnp.any(ids_all[:, :, None] == experts[None, None, :], axis=1)
    masked = jnp.where(named, logits, -jnp.inf)
    raised = jnp.exp(masked - jnp.max(masked, axis=1, keepdims=True))
    share = (raised / jnp.sum(raised, axis=1, keepdims=True)).astype(jnp.bfloat16)
    share_here = lax.dynamic_slice_in_dim(share, place * experts_here, experts_here, 1)
    local = place * experts_here + jnp.arange(experts_here, dtype=jnp.int32)
    named_here = jnp.any(ids_all[:, :, None] == local[None, None, :], axis=1)
    token = jnp.arange(all_tokens, dtype=jnp.int32)
    before = (token[None, :] < token[:, None]).astype(jnp.bfloat16)
    rank = jnp.dot(
        before, named_here.astype(jnp.bfloat16), preferred_element_type=jnp.float32
    ).astype(jnp.int32)
    rank = jnp.where(named_here, rank, -1)
    slot = jnp.arange(slots, dtype=jnp.int32)
    chosen = rank[:, :, None] == slot[None, None, :]
    mixing = jnp.where(chosen, share_here[:, :, None], jnp.zeros((), jnp.bfloat16)).reshape(
        all_tokens, experts_here * slots
    )
    picker = (rank.T[:, None, :] == slot[None, :, None]).astype(jnp.bfloat16)
    picker = picker.reshape(experts_here * slots, all_tokens)
    arrived = (
        jnp.dot(picker, normed, preferred_element_type=jnp.float32)
        .astype(jnp.bfloat16)
        .reshape(experts_here, slots, model_width)
    )
    by_expert = lambda weight: weight.reshape((experts_here, GROUPS) + weight.shape[1:])
    routed = experts_mixed(
        arrived, by_expert(gate_weight), by_expert(up_weight), by_expert(down_weight), mixing
    )

    kept = lax.dynamic_slice_in_dim(routed, core * half_width, half_width, 1)
    given = lax.dynamic_slice_in_dim(routed, (1 - core) * half_width, half_width, 1)
    half_sum = (kept + swap_cores(given.astype(jnp.bfloat16)).astype(jnp.float32)).astype(
        jnp.bfloat16
    )
    rows = [
        lax.dynamic_slice_in_dim(half_sum, (place ^ k) * tokens_here, tokens_here, 0)
        for k in range(width)
    ]
    order = sorted(range(2, width, 2), key=lambda k: -k.bit_length())
    pairs = lambda k: [(i, i ^ k) for i in range(width)]
    received = []
    for k in order + [0]:
        both = rows[k].astype(jnp.float32) + lax.ppermute(rows[k + 1], "ep", pairs(1)).astype(
            jnp.float32
        )
        if k:
            received.append(lax.ppermute(both.astype(jnp.bfloat16), "ep", pairs(k)))
        else:
            total = both
    for block in received:
        total = total + block.astype(jnp.float32)
    return (hidden_part, total.astype(jnp.bfloat16))


def solution(mesh):
    width, cores = mesh.shape["ep"], mesh.shape["tp"]
    gathered = width <= 16 and width & (width - 1) == 0 and width > 1 and cores == 2
    gathered = gathered and PIECES % (width * GROUPS) == 0
    return jax.shard_map(
        body if gathered else wide_body,
        mesh=mesh,
        in_specs=(
            P(("grp", "ep"), "tp", None),
            P(("grp", "ep"), "tp", None),
            P(("grp", "ep"), None),
            P(("grp", "ep")),
            P(("grp", "ep")),
            P("tp", "ep", None),
            P("tp", "ep"),
            P(),
            P(),
            P(("grp", "ep"), None),
            P("ep", None, "tp"),
            P("ep", None, "tp"),
            P("ep", "tp", None),
        ),
        out_specs=(P(("grp", "ep"), "tp"), P(("grp", "ep"), "tp")),
        check_vma=False,
    )
```

```python
import jax
import jax.numpy as jnp
from jax import lax
from jax.experimental import pallas as pl
from jax.experimental.pallas import tpu as pltpu
from jax.sharding import PartitionSpec as P

LATENT = 512
VDIM = 128
EXPERTS = 64
TOPK = 6
GROUPS = 2
CAP = 8
PIECES = 128


score_scale = 192.0 ** (-0.5)
epsilon = 1e-06


def masked_scores(queries, block_rows, token_request, token_visible):
    per_request = block_rows.shape[1]
    flat_rows = block_rows.reshape(-1, block_rows.shape[2])
    scores = (
        jnp.einsum("thc,kc->thk", queries, flat_rows, preferred_element_type=jnp.float32)
        * score_scale
    )
    column = jnp.arange(flat_rows.shape[0], dtype=jnp.int32)
    owner_id = column // per_request
    position = column % per_request
    allowed = (owner_id[None, :] == token_request[:, None]) & (
        position[None, :] < token_visible[:, None]
    )
    return (jnp.where(allowed[:, None, :], scores, -jnp.inf), flat_rows)


def weighted_rows(scores, row_peak, flat_rows):
    weights = jnp.exp(scores - row_peak[:, :, None]).astype(jnp.bfloat16)
    totals = jnp.sum(weights.astype(jnp.float32), axis=2)
    summed = jnp.einsum(
        "thk,kc->thc", weights, flat_rows[:, :LATENT], preferred_element_type=jnp.float32
    )
    return (summed, totals)


def expert_block(arrived, gate_weight, up_weight, down_weight):
    gate_vals = jnp.einsum("prd,pdf->prf", arrived, gate_weight, preferred_element_type=jnp.float32)
    up_vals = jnp.einsum("prd,pdf->prf", arrived, up_weight, preferred_element_type=jnp.float32)
    activated = (jax.nn.silu(gate_vals) * up_vals).astype(jnp.bfloat16)
    return jnp.einsum(
        "prf,pfd->prd", activated, down_weight, preferred_element_type=jnp.float32
    ).astype(jnp.bfloat16)


def wide_body(
    queries,
    latent_cache,
    residual,
    token_request,
    token_visible,
    value_proj,
    out_proj,
    norm_gain,
    router,
    expert_ids,
    gate_weight,
    up_weight,
    down_weight,
):
    all_rows = lax.all_gather(latent_cache, "tp", axis=1, tiled=True)
    scores, flat_rows = masked_scores(queries, all_rows, token_request, token_visible)
    summed, totals = weighted_rows(scores, jnp.max(scores, axis=2), flat_rows)
    context = (summed / totals[:, :, None]).astype(jnp.bfloat16)
    tokens_here = context.shape[0]
    heads_here = context.shape[1]
    head_values = jnp.einsum(
        "thl,hlv->thv",
        context,
        lax.all_gather(value_proj, "ep", axis=1, tiled=True),
        preferred_element_type=jnp.float32,
    )
    heads_out = head_values.astype(jnp.bfloat16).reshape(tokens_here, heads_here * VDIM)
    column_block = jnp.dot(
        lax.all_gather(heads_out, "ep", axis=0, tiled=True),
        out_proj,
        preferred_element_type=jnp.float32,
    )
    attention_part = lax.all_to_all(column_block, "ep", split_axis=0, concat_axis=1, tiled=True)
    attention = lax.psum(attention_part, "tp")
    hidden = (residual.astype(jnp.float32) + attention).astype(jnp.bfloat16)
    hidden_wide = hidden.astype(jnp.float32)
    normed = (
        hidden_wide
        * lax.rsqrt(jnp.mean(hidden_wide * hidden_wide, axis=1, keepdims=True) + epsilon)
        * norm_gain
    ).astype(jnp.bfloat16)
    logits = jnp.dot(normed, router, preferred_element_type=jnp.float32)
    gate_share = jax.nn.softmax(jnp.take_along_axis(logits, expert_ids, axis=1), axis=1).astype(
        jnp.bfloat16
    )
    flat_ids = expert_ids.reshape(-1)
    position_id = jnp.arange(flat_ids.shape[0], dtype=jnp.int32)
    earlier = (flat_ids[:, None] == flat_ids[None, :]) & (
        position_id[None, :] < position_id[:, None]
    )
    slot_ids = (flat_ids * CAP + jnp.sum(earlier.astype(jnp.int32), axis=1)).reshape(
        tokens_here, TOPK
    )
    targets = jnp.arange(EXPERTS * CAP, dtype=jnp.int32)
    matches = slot_ids[:, :, None] == targets[None, None, :]
    picker = jnp.any(matches, axis=1).T.astype(jnp.bfloat16)
    model_width = normed.shape[1]
    mixing = jnp.sum(
        jnp.where(matches, gate_share[:, :, None], jnp.zeros((), jnp.bfloat16)), axis=1
    )
    mixing = jnp.broadcast_to(
        mixing.reshape(tokens_here, EXPERTS, 1, CAP), (tokens_here, EXPERTS, GROUPS, CAP)
    ).reshape(tokens_here, PIECES * CAP)
    core_count = lax.axis_size("tp")
    half_width = model_width // core_count
    core_start = lax.axis_index("tp") * half_width
    outgoing = jnp.dot(picker, normed, preferred_element_type=jnp.float32).astype(jnp.bfloat16)
    outgoing = jnp.broadcast_to(
        outgoing.reshape(EXPERTS, 1, CAP, model_width), (EXPERTS, GROUPS, CAP, model_width)
    ).reshape(PIECES, CAP, model_width)
    arrived = lax.all_to_all(outgoing, "ep", split_axis=0, concat_axis=1, tiled=True)
    partial_out = expert_block(arrived, gate_weight, up_weight, down_weight)
    returned = lax.all_to_all(partial_out, "ep", split_axis=1, concat_axis=0, tiled=True)
    routed = jnp.dot(
        mixing, returned.reshape(PIECES * CAP, model_width), preferred_element_type=jnp.float32
    )
    expert_out = lax.psum_scatter(
        routed.astype(jnp.bfloat16), "tp", scatter_dimension=1, tiled=True
    )
    hidden_part = lax.dynamic_slice_in_dim(hidden, core_start, half_width, 1)
    return (hidden_part, expert_out)


def relative_blocks(block, width):
    pairs = lambda k: [(i, i ^ k) for i in range(width)]
    blocks = [None] * width
    blocks[0] = block
    order = sorted(range(2, width, 2), key=lambda k: -k.bit_length())
    for k in order:
        blocks[k] = lax.ppermute(block, "ep", pairs(k))
    for k in [0] + order:
        blocks[k + 1] = lax.ppermute(blocks[k], "ep", pairs(1))
    return blocks


def place_blocks(groups, axis, place, core):
    blocks = [block for group in groups for block in group]
    width, sides = len(groups[0]), len(groups)
    size = blocks[0].shape[axis]
    shape = list(blocks[0].shape)
    shape[axis] = size * len(blocks)

    def kernel(where, *refs):
        out = refs[-1]
        for side in range(sides):
            for k in range(width):
                slot = where[0] ^ k
                if sides > 1:
                    slot = slot * sides + (where[1] ^ side)
                index = [slice(None)] * len(shape)
                index[axis] = pl.ds(pl.multiple_of(slot * size, size), size)
                out[tuple(index)] = refs[side * width + k][...]

    vmem = pl.BlockSpec(memory_space=pltpu.VMEM)
    return pl.pallas_call(
        kernel,
        out_shape=jax.ShapeDtypeStruct(tuple(shape), blocks[0].dtype),
        in_specs=[pl.BlockSpec(memory_space=pltpu.SMEM)] + [vmem] * len(blocks),
        out_specs=vmem,
    )(jnp.stack([place, core]).astype(jnp.int32), *blocks)


def pack_early(residual, ids_rows, width, place, core):
    tokens_here, model_width = residual.shape
    extra, lanes = ids_rows.shape
    rows = tokens_here + extra

    def kernel(where, residual_ref, ids_ref, even, odd):
        for k in range(width):
            start = ((where[0] ^ k) * 2 + where[1]) * lanes
            target = odd if k % 2 else even
            target[k // 2, :tokens_here, :] = residual_ref[:, pl.ds(pl.multiple_of(start, lanes), lanes)]
            target[k // 2, tokens_here:, :] = ids_ref[...]

    vmem = pl.BlockSpec(memory_space=pltpu.VMEM)
    shape = jax.ShapeDtypeStruct((width // 2, rows, lanes), residual.dtype)
    return pl.pallas_call(
        kernel,
        out_shape=(shape, shape),
        in_specs=[pl.BlockSpec(memory_space=pltpu.SMEM), vmem, vmem],
        out_specs=(vmem, vmem),
    )(jnp.stack([place, core]).astype(jnp.int32), residual, ids_rows)


def project_blocks(blocks, out_proj, place, core):
    rows, width = blocks[0].shape[0], len(blocks)
    half = out_proj.shape[1] // 2

    def kernel(where, proj, *refs):
        kept, given = refs[width:]
        mine = pl.ds(pl.multiple_of(where[1] * half, half), half)
        theirs = pl.ds(pl.multiple_of((1 - where[1]) * half, half), half)
        stacked = jnp.concatenate([ref[...] for ref in refs[:width]], axis=0)
        for target, columns in ((kept, mine), (given, theirs)):
            result = jnp.dot(stacked, proj[:, columns], preferred_element_type=jnp.float32)
            for k in range(width):
                slot = pl.multiple_of((where[0] ^ k) * rows, rows)
                target[pl.ds(slot, rows), :] = result[k * rows : (k + 1) * rows]

    vmem = pl.BlockSpec(memory_space=pltpu.VMEM)
    shape = jax.ShapeDtypeStruct((rows * width, half), jnp.float32)
    return pl.pallas_call(
        kernel,
        out_shape=(shape, shape),
        in_specs=[pl.BlockSpec(memory_space=pltpu.SMEM)] + [vmem] * (width + 1),
        out_specs=(vmem, vmem),
    )(jnp.stack([place, core]).astype(jnp.int32), out_proj, *blocks)


def mix_half(mixing, slots_out, side, dtype):
    half = slots_out.shape[1] // 2

    def kernel(where, mixing_ref, slots_ref, out):
        columns = pl.ds(pl.multiple_of(where[0] * half, half), half)
        out[...] = jnp.dot(
            mixing_ref[...], slots_ref[:, columns], preferred_element_type=jnp.float32
        ).astype(dtype)

    vmem = pl.BlockSpec(memory_space=pltpu.VMEM)
    return pl.pallas_call(
        kernel,
        out_shape=jax.ShapeDtypeStruct((mixing.shape[0], half), dtype),
        in_specs=[pl.BlockSpec(memory_space=pltpu.SMEM), vmem, vmem],
        out_specs=vmem,
    )(side[None].astype(jnp.int32), mixing, slots_out)


def sum_relative(kept, taken, width, place, first):
    rows = kept.shape[0] // width

    def kernel(where, kept_ref, taken_ref, *outs):
        for k in range(first, width, 2):
            part = pl.ds(pl.multiple_of((where[0] ^ k) * rows, rows), rows)
            outs[k // 2][...] = (
                kept_ref[part, :] + taken_ref[part, :].astype(jnp.float32)
            ).astype(jnp.bfloat16)

    vmem = pl.BlockSpec(memory_space=pltpu.VMEM)
    shape = jax.ShapeDtypeStruct((rows, kept.shape[1]), jnp.bfloat16)
    return pl.pallas_call(
        kernel,
        out_shape=(shape,) * (width // 2),
        in_specs=[pl.BlockSpec(memory_space=pltpu.SMEM), vmem, vmem],
        out_specs=(vmem,) * (width // 2),
    )(place[None].astype(jnp.int32), kept, taken)


def add_blocks(blocks):
    def kernel(*refs):
        total = refs[0][...].astype(jnp.float32)
        for ref in refs[1:-1]:
            total = total + ref[...].astype(jnp.float32)
        refs[-1][...] = total.astype(jnp.bfloat16)

    vmem = pl.BlockSpec(memory_space=pltpu.VMEM)
    return pl.pallas_call(
        kernel,
        out_shape=jax.ShapeDtypeStruct(blocks[0].shape, jnp.bfloat16),
        in_specs=[vmem] * len(blocks),
        out_specs=vmem,
    )(*blocks)


def expert_kernel(arrived, gate_ref, up_ref, down_ref, out):
    rows = arrived[0]
    hidden_units = gate_ref.shape[0] * gate_ref.shape[1]
    width = rows.shape[1]
    turned = (((1,), (1,)), ((), ()))
    gate_vals = lax.dot_general(
        rows, gate_ref[...].reshape(hidden_units, width), turned, preferred_element_type=jnp.float32
    )
    up_vals = lax.dot_general(
        rows, up_ref[...].reshape(hidden_units, width), turned, preferred_element_type=jnp.float32
    )
    activated = (gate_vals / (1.0 + jnp.exp(-gate_vals)) * up_vals).astype(jnp.bfloat16)
    out[...] = jnp.dot(
        activated, down_ref[...].reshape(hidden_units, width), preferred_element_type=jnp.float32
    ).astype(jnp.bfloat16)


def run_experts(arrived, gate_weight, up_weight, down_weight):
    experts_here, slots, width = arrived.shape
    units = down_weight.shape[1]
    weight = pl.BlockSpec((GROUPS, units, width), lambda x: (x, 0, 0))
    return pl.pallas_call(
        expert_kernel,
        grid=(experts_here,),
        out_shape=jax.ShapeDtypeStruct((experts_here * slots, width), jnp.bfloat16),
        in_specs=[pl.BlockSpec((1, slots, width), lambda x: (x, 0, 0)), weight, weight, weight],
        out_specs=pl.BlockSpec((slots, width), lambda x: (x, 0)),
    )(arrived, jnp.swapaxes(gate_weight, 1, 2), jnp.swapaxes(up_weight, 1, 2), down_weight)


def swap_cores(value):
    return lax.ppermute(value, "tp", [(0, 1), (1, 0)])


def body(
    queries,
    latent_cache,
    residual,
    token_request,
    token_visible,
    value_proj,
    out_proj,
    norm_gain,
    router,
    expert_ids,
    gate_weight,
    up_weight,
    down_weight,
):
    width = lax.axis_size("ep")
    place = lax.axis_index("ep")
    core = lax.axis_index("tp")
    tokens_here, model_width = residual.shape
    all_tokens = tokens_here * width
    columns = out_proj.shape[1]
    half_columns = columns // 2
    half_width = model_width // 2

    other_rows = swap_cores(latent_cache)
    requests, positions, latent_width = latent_cache.shape
    value_blocks = relative_blocks(value_proj, width)

    pairs = lambda k: [(i, i ^ k) for i in range(width)]
    ids_rows = jnp.pad(
        expert_ids.T.astype(jnp.bfloat16), ((0, 8 - TOPK), (0, half_columns - tokens_here))
    )
    even, odd = pack_early(residual, ids_rows, width, place, core)
    crossed = lax.ppermute(odd, "ep", pairs(1))
    both = jnp.stack([even, crossed], axis=1)
    early = [both[0]] + [lax.ppermute(both[i], "ep", pairs(2 * i)) for i in range(1, width // 2)]
    def half_scores(rows, source_core):
        flat = rows.reshape(requests * positions, latent_width)
        scores = (
            jnp.einsum("thc,kc->thk", queries, flat, preferred_element_type=jnp.float32)
            * score_scale
        )
        column = jnp.arange(requests * positions, dtype=jnp.int32)
        position = column % positions + source_core * positions
        allowed = ((column // positions)[None, :] == token_request[:, None]) & (
            position[None, :] < token_visible[:, None]
        )
        return jnp.where(allowed[:, None, :], scores, -jnp.inf), flat

    own_scores, own_flat = half_scores(latent_cache, core)
    far_scores, far_flat = half_scores(other_rows, 1 - core)
    row_peak = jnp.maximum(jnp.max(own_scores, axis=2), jnp.max(far_scores, axis=2))
    own_sum, own_total = weighted_rows(own_scores, row_peak, own_flat)
    far_sum, far_total = weighted_rows(far_scores, row_peak, far_flat)
    context = ((own_sum + far_sum) / (own_total + far_total)[:, :, None]).astype(jnp.bfloat16)
    heads_here = context.shape[1]
    value_blocks, context, early = lax.optimization_barrier((value_blocks, context, early))
    value_full = place_blocks([value_blocks], 1, place, core)
    head_values = jnp.einsum(
        "thl,hlv->thv", context, value_full, preferred_element_type=jnp.float32
    )
    heads_out = head_values.astype(jnp.bfloat16).reshape(tokens_here, heads_here * VDIM)
    early = place_blocks([[part[q : q + 1] for part in early for q in range(2)]], 0, place, core)
    residual_columns = early[:, :tokens_here].reshape(all_tokens, half_columns)
    ids_all = (
        early[:, tokens_here : tokens_here + TOPK, :tokens_here]
        .transpose(0, 2, 1)
        .reshape(all_tokens, TOPK)
        .astype(jnp.int32)
    )
    head_blocks, residual_columns, ids_all = lax.optimization_barrier(
        (relative_blocks(heads_out, width), residual_columns, ids_all)
    )
    kept, given = project_blocks(head_blocks, out_proj, place, core)
    hidden_columns = (
        residual_columns.astype(jnp.float32) + (kept + swap_cores(given))
    ).astype(jnp.bfloat16)

    own_half = relative_blocks(hidden_columns, width)
    other_half = [swap_cores(block) for block in own_half]
    hidden = place_blocks([own_half, other_half], 1, place, core)
    hidden_part = lax.dynamic_slice(
        hidden, (place * tokens_here, core * half_width), (tokens_here, half_width)
    )
    hidden_wide = hidden.astype(jnp.float32)
    normed = (
        hidden_wide
        * lax.rsqrt(jnp.mean(hidden_wide * hidden_wide, axis=1, keepdims=True) + epsilon)
        * norm_gain
    ).astype(jnp.bfloat16)

    experts_here = gate_weight.shape[0] // GROUPS
    slots = CAP * width
    logits = jnp.dot(normed, router, preferred_element_type=jnp.float32)
    experts = jnp.arange(EXPERTS, dtype=jnp.int32)
    named = jnp.any(ids_all[:, :, None] == experts[None, None, :], axis=1)
    masked = jnp.where(named, logits, -jnp.inf)
    raised = jnp.exp(masked - jnp.max(masked, axis=1, keepdims=True))
    share = (raised / jnp.sum(raised, axis=1, keepdims=True)).astype(jnp.bfloat16)
    share_here = lax.dynamic_slice_in_dim(share, place * experts_here, experts_here, 1)
    local = place * experts_here + jnp.arange(experts_here, dtype=jnp.int32)
    named_here = jnp.any(ids_all[:, :, None] == local[None, None, :], axis=1)
    token = jnp.arange(all_tokens, dtype=jnp.int32)
    before = (token[None, :] < token[:, None]).astype(jnp.bfloat16)
    rank = jnp.dot(
        before, named_here.astype(jnp.bfloat16), preferred_element_type=jnp.float32
    ).astype(jnp.int32)
    rank = jnp.where(named_here, rank, -1)
    slot = jnp.arange(slots, dtype=jnp.int32)
    chosen = rank[:, :, None] == slot[None, None, :]
    mixing = jnp.where(chosen, share_here[:, :, None], jnp.zeros((), jnp.bfloat16)).reshape(
        all_tokens, experts_here * slots
    )
    picker = (rank.T[:, None, :] == slot[None, :, None]).astype(jnp.bfloat16)
    picker = picker.reshape(experts_here * slots, all_tokens)
    arrived = (
        jnp.dot(picker, normed, preferred_element_type=jnp.float32)
        .astype(jnp.bfloat16)
        .reshape(experts_here, slots, model_width)
    )
    slots_out = run_experts(arrived, gate_weight, up_weight, down_weight)
    given = mix_half(mixing, slots_out, 1 - core, jnp.bfloat16)
    taken = swap_cores(given)
    kept = mix_half(mixing, slots_out, core, jnp.float32)
    odd = sum_relative(kept, taken, width, place, 1)
    even = sum_relative(kept, taken, width, place, 0)
    rows = [block for two in zip(even, odd) for block in two]
    order = sorted(range(2, width, 2), key=lambda k: -k.bit_length())
    crossed = {k: lax.ppermute(rows[k + 1], "ep", pairs(1)) for k in order + [0]}
    received = [
        lax.ppermute(add_blocks([rows[k], crossed[k]]), "ep", pairs(k)) for k in order
    ]
    total = add_blocks([rows[0], crossed[0]] + received)
    return (hidden_part, total)


def solution(mesh):
    width, cores = mesh.shape["ep"], mesh.shape["tp"]
    gathered = width <= 16 and width & (width - 1) == 0 and width > 1 and cores == 2
    gathered = gathered and PIECES % (width * GROUPS) == 0
    return jax.shard_map(
        body if gathered else wide_body,
        mesh=mesh,
        in_specs=(
            P(("grp", "ep"), "tp", None),
            P(("grp", "ep"), "tp", None),
            P(("grp", "ep"), None),
            P(("grp", "ep")),
            P(("grp", "ep")),
            P("tp", "ep", None),
            P("tp", "ep"),
            P(),
            P(),
            P(("grp", "ep"), None),
            P("ep", None, "tp"),
            P("ep", None, "tp"),
            P("ep", "tp", None),
        ),
        out_specs=(P(("grp", "ep"), "tp"), P(("grp", "ep"), "tp")),
        check_vma=False,
    )
```
